32 devices in a mesh: dom: 16 (over z, y, core), sub: 2 (over x).
Axes of the slice: x: 2, y: 2, z: 4, core: 2. Of those that a mesh axis runs over, the one named last changes fastest.
Arguments:
- fine_partial: float32 [2, 165, 2048], P('sub', None, 'dom'), may hold values from -6 to 6
- upward_ops: float32 [8, 165, 165], replicated, may hold values from -0.15625 to 0.15625
- interaction_ops: float32 [188, 165, 165], P('sub'), may hold values from -0.03125 to 0.03125
- downward_ops: float32 [8, 165, 165], replicated, may hold values from -0.5 to 0.5
- fine_list: int32 [188, 2048], P('sub', 'dom'), may hold values from -1 to 2047, as said below
- mid_list: int32 [188, 256], P('sub', 'dom'), may hold values from -1 to 255, as said below
- top_list: int32 [188, 32], P('sub', 'dom'), may hold values from -1 to 31, as said below
- upper_list: int32 [188, 4], P('sub'), may hold values from -1 to 3, as said below
- positions: float32 [3, 65536], P(None, ('dom', 'sub')), may hold values from -0.5 to 0.5
- leaf_cell: int32 [65536], P(('dom', 'sub')), may hold values from 0 to 2047, as said below
Outputs:
- local_fine: float32 [165, 2048], P(None, 'dom')
- potential: float32 [65536], P(('dom', 'sub'))
The draws below stay inside these ranges and needn't reach their ends.
Inputs may be any that keep to these rules, and one draw needn't show every extreme that they name: `fine_list`: column t lists for each offset slot a cell of the finest level within 128 cells of t in Peano order, or -1 for an empty slot. `mid_list`: column t lists for each offset slot a cell of the middle level within 16 cells of t, or -1 for an empty slot. `top_list`: each entry is a cell of the top level, or -1 for an empty slot. `upper_list`: each entry is a cell of the upper level, or -1 for an empty slot. `leaf_cell`: A particle's leaf is one of the 128 finest cells owned by its own slab.
All inputs are finite; a program needn't handle non-finite values.
Results may differ from the reference program's by a relative error of at most 0.0003.
Values sent between devices are 32-bit elements; how exact they have to be, the bound alone decides.
A program may use at most 128 MiB of HBM per device.

```python
import jax
import jax.numpy as jnp
from jax import lax

ORDER = 8
NC = 165
NOFF = 188
CF = 128
NF = 2048
NM = 256
NT = 32
NU = 4
PARTICLES = 65536
N_DOM = 16
N_SUB = 2


def window_list(key, cells_total, reach):
    targets = jnp.arange(cells_total, dtype=jnp.int32)[None, :]
    offsets = jax.random.randint(key, (NOFF, cells_total), -reach, reach + 1, dtype=jnp.int32)
    sources = targets + offsets
    inside = (sources >= 0) & (sources < cells_total)
    return jnp.where(inside, sources, -1).astype(jnp.int32)


def global_list(key, cells_total):
    key_one, key_two = jax.random.split(key)
    drawn_cells = jax.random.randint(key_one, (NOFF, cells_total), 0, cells_total, dtype=jnp.int32)
    vacant = jax.random.randint(key_two, (NOFF, cells_total), 0, 8, dtype=jnp.int32) == 0
    return jnp.where(vacant, -1, drawn_cells).astype(jnp.int32)


def draw_fine_list(key, part):
    return window_list(jax.random.fold_in(key, 11), NF, CF)


def draw_mid_list(key, part):
    return window_list(jax.random.fold_in(key, 12), NM, CF // 8)


def draw_top_list(key, part):
    return global_list(jax.random.fold_in(key, 13), NT)


def draw_upper_list(key, part):
    return global_list(jax.random.fold_in(key, 14), NU)


def draw_leaf_cell(key, part):
    slabs = NF // CF
    indices = jnp.arange(PARTICLES, dtype=jnp.int32)
    slab_index = indices // (PARTICLES // slabs)
    inner = jax.random.randint(jax.random.fold_in(key, 15), (PARTICLES,), 0, CF, dtype=jnp.int32)
    return (slab_index * CF + inner).astype(jnp.int32)


def level_of(stream_key, extent, shards, smallest, top_value):
    gain, own = 1.0, jax.random.fold_in(stream_key, 6)
    for position, blocks in shards:
        draws = jnp.exp(jax.random.uniform(jax.random.fold_in(own, position), (blocks,), jnp.float32, smallest / len(shards), top_value / len(shards)))
        gain = gain * jnp.repeat(draws, extent[position] // blocks).reshape([-1 if axis == position else 1 for axis in range(len(extent))])
    return gain


def noise(key, dims, scale, most, pieces=(), kind=jnp.bfloat16):
    result = scale * jax.random.normal(key, dims, jnp.float32)
    if pieces:
        result = result * level_of(key, dims, pieces, -0.22, 0.18)
    return jnp.clip(result, -most, most).astype(kind)


def setup_inputs(seed: int = 0) -> dict:
    splits = jax.random.split(jax.random.key(seed), 11)
    return {
        "fine_partial": noise(splits[0], (N_SUB, NC, NF), 1.0, 6.0, ((0, 2), (2, 16)), jnp.float32),
        "upward_ops": noise(splits[1], (8, NC, NC), (8 * NC) ** -0.5, 0.15625, (), jnp.float32),
        "interaction_ops": noise(splits[2], (NOFF, NC, NC), (NOFF * NC) ** -0.5, 0.03125, ((0, 2),), jnp.float32),
        "downward_ops": noise(splits[3], (8, NC, NC), NC ** -0.5, 0.5, (), jnp.float32),
        "fine_list": draw_fine_list(jax.random.fold_in(splits[10], 71), 0),
        "mid_list": draw_mid_list(jax.random.fold_in(splits[10], 71), 0),
        "top_list": draw_top_list(jax.random.fold_in(splits[10], 71), 0),
        "upper_list": draw_upper_list(jax.random.fold_in(splits[10], 71), 0),
        "positions": jnp.clip(jax.random.uniform(splits[8], (3, PARTICLES), jnp.float32, -0.5, 0.5) * level_of(splits[8], (3, PARTICLES), ((1, 32),), -0.4, 0.0), -0.5, 0.5),
        "leaf_cell": draw_leaf_cell(jax.random.fold_in(splits[10], 71), 0),
    }


precise = lax.Precision.HIGHEST


def exponents():
    entries = []
    for degree in range(ORDER + 1):
        for along_x in range(degree, -1, -1):
            for along_y in range(degree - along_x, -1, -1):
                entries.append((along_x, along_y, degree - along_x - along_y))
    return entries


def monomials(coords):
    powers = [jnp.ones_like(coords)]
    for degree in range(ORDER):
        powers.append(powers[-1] * coords)
    rows = []
    for triple in exponents():
        rows.append(powers[triple[0]][0] * powers[triple[1]][1] * powers[triple[2]][2])
    return jnp.stack(rows)


def upward(moments, upward_ops):
    parents = moments.shape[1] // 8
    grouped = moments.reshape(moments.shape[0], parents, 8)
    return jnp.einsum("oab,bpo->ap", upward_ops, grouped, precision=precise)


def downward(expansions, downward_ops):
    spread = jnp.einsum("oab,bp->apo", downward_ops, expansions, precision=precise)
    return spread.reshape(spread.shape[0], -1)


def interact(moments, sources, interaction_ops, block_size):
    targets = sources.shape[1]

    def one_block(block_index):
        chosen = lax.dynamic_slice_in_dim(sources, block_index * block_size, block_size, 1)
        present = chosen >= 0
        picked = jnp.take(moments, jnp.clip(chosen, 0, moments.shape[1] - 1), axis=1)
        picked = jnp.where(present[None], picked, jnp.float32(0.0))
        return jnp.einsum("jab,bjt->at", interaction_ops, picked, precision=precise)

    results = lax.map(one_block, jnp.arange(targets // block_size, dtype=jnp.int32))
    return jnp.transpose(results, (1, 0, 2)).reshape(moments.shape[0], targets)


def reference(fine_partial, upward_ops, interaction_ops, downward_ops, fine_list, mid_list, top_list, upper_list, positions, leaf_cell):
    fine_moments = jnp.sum(fine_partial, axis=0)
    mid_moments = upward(fine_moments, upward_ops)
    top_moments = upward(mid_moments, upward_ops)
    upper_moments = upward(top_moments, upward_ops)
    local_upper = interact(upper_moments, upper_list, interaction_ops, upper_moments.shape[1])
    local_top = interact(top_moments, top_list, interaction_ops, CF // 64) + downward(local_upper, downward_ops)
    local_mid = interact(mid_moments, mid_list, interaction_ops, CF // 8) + downward(local_top, downward_ops)
    local_fine = interact(fine_moments, fine_list, interaction_ops, CF) + downward(local_mid, downward_ops)
    slab_span = PARTICLES // N_DOM

    def slab_potential(slab_index):
        coords = lax.dynamic_slice_in_dim(positions, slab_index * slab_span, slab_span, 1)
        leaves = lax.dynamic_slice_in_dim(leaf_cell, slab_index * slab_span, slab_span, 0)
        columns = jnp.take(local_fine, leaves, axis=1)
        return jnp.sum(columns * monomials(coords), axis=0)

    potential = lax.map(slab_potential, jnp.arange(N_DOM, dtype=jnp.int32)).reshape(-1)
    return local_fine, potential
```

```python
import functools

import jax
import jax.numpy as jnp
from jax import lax
from jax.experimental import pallas as pl
from jax.experimental.pallas import tpu as pltpu
from jax.sharding import PartitionSpec as P

ORDER = 8
LANES = 128


precise = lax.Precision.HIGHEST


def round_up(count, unit):
    return -(-count // unit) * unit


def exponents():
    entries = []
    for degree in range(ORDER + 1):
        for along_x in range(degree, -1, -1):
            for along_y in range(degree - along_x, -1, -1):
                entries.append((along_x, along_y, degree - along_x - along_y))
    return entries


def halves(value):
    high = value.astype(jnp.bfloat16)
    low = (value - high.astype(jnp.float32)).astype(jnp.bfloat16)
    return high, low


def one_hot(row, count):
    places = lax.broadcasted_iota(jnp.int32, (count, row.shape[1]), 0)
    return jnp.where(places == row, 1.0, 0.0).astype(jnp.bfloat16)


def matmul(left, right):
    return jnp.dot(left, right, preferred_element_type=jnp.float32)


def one_hot_blocks(row, blocks):
    places = lax.broadcasted_iota(jnp.int32, (LANES, LANES), 0)
    places = places.astype(jnp.float32).astype(jnp.bfloat16)
    pieces = []
    for m in range(blocks):
        wanted = jnp.broadcast_to(row - float(LANES * m), (LANES, LANES)).astype(jnp.bfloat16)
        one, zero = jnp.ones((), jnp.bfloat16), jnp.zeros((), jnp.bfloat16)
        pieces.append(jnp.where(places == wanted, one, zero))
    return jnp.concatenate(pieces, axis=0)


def operator_copy(ops_ref, stage, arrived, part):
    coeffs = ops_ref.shape[0]
    count = min(8, coeffs - 8 * part)
    return pltpu.make_async_copy(
        ops_ref.at[:, pl.ds(8 * part, count), :],
        stage.at[part, :, pl.ds(0, count), :],
        arrived.at[part],
    )


def interact_kernel(
    spread, tops, fine_ref, tops_ref, upward_ref, fine_list, coarse_list, ops_ref, out_ref,
    stage, fine_table, coarse_table, fine_picked, coarse_picked, lists, held, arrived,
):
    rows = fine_ref.shape[0]
    coeffs, _, slots = ops_ref.shape
    depth = fine_list.shape[0]
    width = coarse_table.shape[1] // 2
    stride = fine_picked.shape[0] // rows
    parts = stage.shape[0]
    for part in range(parts):
        operator_copy(ops_ref, stage, arrived, part).start()

    ops_high, ops_low = split_upward(upward_ref, held)

    def shifted(value, amount):
        extra = width - value.shape[1]
        if extra:
            filler = jnp.zeros((rows, extra), jnp.float32)
            value = jnp.concatenate([value, filler], axis=1)
        return pltpu.roll(value, amount, 1) if amount else value

    top_moments = jnp.transpose(tops_ref[...])[:rows]
    coarse = shifted(raise_level(fine_ref[...], ops_high, ops_low), 0)
    coarse += shifted(top_moments, spread)
    coarse += shifted(raise_level(top_moments, ops_high, ops_low), spread + tops)
    coarse_table[...] = jnp.concatenate(halves(coarse), axis=1)
    high, low = halves(fine_ref[...])
    fine_table[0] = high[:, : 2 * LANES]
    fine_table[1] = low[:, : 2 * LANES]
    fine_table[2] = jnp.concatenate([high[:, 2 * LANES :], low[:, 2 * LANES :]], axis=1)
    lists[0] = fine_list[...].astype(jnp.float32)
    lists[1] = coarse_list[...].astype(jnp.float32)

    for slot in range(0, depth, 2):
        pair = [one_hot_blocks(lists[0, slot + m : slot + m + 1, :], 3) for m in range(2)]
        chosen = jnp.concatenate(pair, axis=1)
        near, far = chosen[: 2 * LANES], chosen[2 * LANES :]
        value = matmul(fine_table[0], near) + matmul(fine_table[1], near)
        value += matmul(fine_table[2], jnp.concatenate([far, far], axis=0))
        pair = [
            one_hot_blocks(lists[1, slot + m : slot + m + 1, :], width // LANES) for m in range(2)
        ]
        chosen = jnp.concatenate(pair, axis=1)
        coarse_value = matmul(coarse_table[...], jnp.concatenate([chosen, chosen], axis=0))
        for m in range(2):
            columns = slice(m * LANES, (m + 1) * LANES)
            fine_picked[pl.ds(slot + m, rows, stride), :] = value[:, columns]
            coarse_picked[pl.ds(slot + m, rows, stride), :] = coarse_value[:, columns]

    for part in range(parts):
        operator_copy(ops_ref, stage, arrived, part).wait()
    below = jnp.zeros((LANES - depth, 2 * LANES), jnp.bfloat16)
    beside = jnp.zeros((coeffs, LANES - slots), jnp.float32)
    under = jnp.zeros((rows - coeffs, LANES), jnp.float32)
    total = None
    for first in range(0, coeffs, 24):
        left = []
        right = []
        for term in range(first, min(first + 24, coeffs)):
            block = stage.at[term // 8].reshape(coeffs * 8, slots)
            op = block[pl.ds(term % 8, coeffs, 8), :]
            op = jnp.concatenate([jnp.concatenate([op, beside], axis=1), under], axis=0)
            op_high, op_low = halves(op)
            place = pl.ds(term * stride, depth)
            data = jnp.concatenate([fine_picked[place, :], coarse_picked[place, :]], axis=1)
            high, low = halves(data)
            high = jnp.concatenate([high, below], axis=0)
            low = jnp.concatenate([low, below], axis=0)
            left += [op_high, op_high, op_low]
            right += [high, low, high]
        product = matmul(jnp.concatenate(left, axis=1), jnp.concatenate(right, axis=0))
        total = product if total is None else total + product
    out_ref[...] = total


def interact(fine, tops_rows, upward_ops, fine_list, coarse_list, ops, spread, tops, coarse_width):
    coeffs, _, slots = ops.shape
    rows, width = fine.shape
    depth = fine_list.shape[0]
    stride = depth + 8
    parts = round_up(coeffs, 8) // 8
    vmem = pl.BlockSpec(memory_space=pltpu.VMEM)
    return pl.pallas_call(
        functools.partial(interact_kernel, spread, tops),
        in_specs=[vmem] * 5 + [pl.BlockSpec(memory_space=pl.ANY)],
        out_specs=vmem,
        out_shape=jax.ShapeDtypeStruct((rows, 2 * LANES), jnp.float32),
        scratch_shapes=[
            pltpu.VMEM((parts, coeffs, 8, slots), jnp.float32),
            pltpu.VMEM((3, rows, 2 * LANES), jnp.bfloat16),
            pltpu.VMEM((rows, 2 * coarse_width), jnp.bfloat16),
            pltpu.VMEM((rows * stride, LANES), jnp.float32),
            pltpu.VMEM((rows * stride, LANES), jnp.float32),
            pltpu.VMEM((2, depth, LANES), jnp.float32),
            pltpu.VMEM((rows, 8, 2 * LANES), jnp.float32),
            pltpu.SemaphoreType.DMA((parts,)),
        ],
        compiler_params=pltpu.CompilerParams(vmem_limit_bytes=52 * 1024 * 1024),
        cost_estimate=pl.CostEstimate(
            flops=6 * rows * rows * LANES * 2 * LANES,
            bytes_accessed=4 * rows * rows * LANES,
            transcendentals=0,
        ),
    )(fine, tops_rows, jnp.transpose(upward_ops, (1, 0, 2)), fine_list, coarse_list, ops)


def potential_kernel(local_ref, leaf_ref, position_ref, exponent_ref, out_ref):
    rows, cells = local_ref.shape
    particles = leaf_ref.shape[1]
    high, low = halves(local_ref[...])
    table = jnp.concatenate([high, low], axis=0)
    masks = [
        [(exponent_ref[:, axis : axis + 1] // bit) % 2 == 1 for bit in (1, 2, 4, 8)]
        for axis in range(3)
    ]
    for start in range(0, particles, 2 * LANES):
        span = slice(start, start + 2 * LANES)
        chosen = one_hot(leaf_ref[:, span], cells)
        both = jnp.dot(table, chosen, preferred_element_type=jnp.float32)
        value = both[:rows] + both[rows:]
        for axis in range(3):
            power = position_ref[axis : axis + 1, span]
            for bit in range(4):
                value = value * jnp.where(masks[axis][bit], power, 1.0)
                power = power * power
        out_ref[:, span] = jnp.sum(value, axis=0, keepdims=True)


def evaluate(local, leaves, positions):
    rows = local.shape[0]
    table = jnp.asarray(exponents(), jnp.int32)
    table = jnp.pad(table, ((0, rows - table.shape[0]), (0, LANES - 3)))
    return pl.pallas_call(
        potential_kernel,
        out_shape=jax.ShapeDtypeStruct((1, leaves.shape[0]), jnp.float32),
        compiler_params=pltpu.CompilerParams(vmem_limit_bytes=32 * 1024 * 1024),
    )(local, leaves[None], positions, table)[0]


def raise_level(moments, ops_high, ops_low):
    rows, width = moments.shape
    parents = round_up(width // 8, LANES)
    high, low = halves(moments)
    source = lax.broadcasted_iota(jnp.int32, (width, 8 * parents), 0)
    target = lax.broadcasted_iota(jnp.int32, (width, 8 * parents), 1)
    wanted = 8 * (target % parents) + target // parents
    chosen = jnp.where(source == wanted, 1.0, 0.0).astype(jnp.bfloat16)
    both = jnp.dot(
        jnp.concatenate([high, low], axis=0), chosen, preferred_element_type=jnp.float32
    )
    filler = jnp.zeros((2 * LANES - rows, parents), jnp.float32)
    stacks = []
    for first in (0, rows):
        pieces = []
        for o in range(8):
            pieces += [both[first : first + rows, o * parents : (o + 1) * parents], filler]
        stacks.append(jnp.concatenate(pieces, axis=0).astype(jnp.bfloat16))
    dot = functools.partial(jnp.dot, preferred_element_type=jnp.float32)
    return dot(ops_high, stacks[0]) + dot(ops_high, stacks[1]) + dot(ops_low, stacks[0])


def split_upward(upward_ref, held):
    coeffs = upward_ref.shape[0]
    held[...] = jnp.zeros_like(held)
    held[:coeffs, :, :coeffs] = upward_ref[...]
    ops = jnp.swapaxes(held[...], 0, 1)
    return halves(jnp.concatenate([ops[o] for o in range(8)], axis=1))


def prepare(
    counts, partial_ref, upward_ref, fine_ref, mid_ref, top_ref, upper_ref,
    rows_out, fine_out, coarse_out, held, lists,
):
    rows = held.shape[0]
    coeffs = partial_ref.shape[0]
    slots = fine_ref.shape[0]
    slab, mid, top, spread, tops = counts
    domain = lax.axis_index("dom")
    filler = jnp.zeros((rows - coeffs, partial_ref.shape[1]), jnp.float32)
    block = jnp.concatenate([partial_ref[...], filler], axis=0)
    high, low = split_upward(upward_ref, held)
    top_moments = raise_level(raise_level(block, high, low), high, low)
    filler = jnp.zeros((2 * LANES - rows, LANES), jnp.float32)
    turned = jnp.transpose(jnp.concatenate([top_moments, filler], axis=0))
    rows_out[...] = turned[: rows_out.shape[0]]

    def place(sources, offset):
        return jnp.where(sources >= 0, sources + offset, -1)

    fine_out[...] = jnp.full_like(fine_out, -1)
    fine_out[:slots, :] = place(fine_ref[...], slab - domain * slab)
    lists[...] = jnp.full_like(lists, -1.0)
    start = 0
    for part in (
        place(mid_ref[...], mid - domain * mid),
        place(top_ref[...], spread),
        place(upper_ref[pl.ds(domain * top // 8, 1), :], spread + tops),
    ):
        lists[start : start + part.shape[0], :slots] = part.astype(jnp.float32)
        start += part.shape[0]
    coarse = jnp.transpose(lists[...])
    coarse_out[...] = coarse[: coarse_out.shape[0]].astype(jnp.int32)


def exchange_kernel(
    domains, subs, counts, block_ref, partial_ref, upward_ref, fine_ref, mid_ref, top_list_ref,
    upper_ref, wide_out, tops_out, fine_out, coarse_out,
    low, high, tops, top_ref, held, lists, side_send, side_recv, top_send, top_recv,
):
    domain, sub = lax.axis_index("dom"), lax.axis_index("sub")
    count = domains * subs
    flat = domain * subs + sub
    mesh = pl.DeviceIdType.MESH
    coeffs, cells = block_ref.shape
    top_cells = top_ref.shape[0]

    def peer(offset):
        place = lax.rem(flat + offset, count)
        return {"dom": place // subs, "sub": lax.rem(place, subs)}

    barrier = pltpu.get_barrier_semaphore()

    def greet(offset, carry):
        pl.semaphore_signal(barrier, inc=1, device_id=peer(offset), device_id_type=mesh)
        return carry

    lax.fori_loop(1, count, greet, 0)
    prepare(
        counts, partial_ref, upward_ref, fine_ref, mid_ref, top_list_ref, upper_ref,
        top_ref, fine_out, coarse_out, held, lists,
    )
    tops[count - 1] = top_ref[...]
    tops_out[...] = jnp.zeros_like(tops_out)
    wide_out[...] = jnp.zeros_like(wide_out)
    wide_out[:coeffs, cells : 2 * cells] = block_ref[...]
    pl.semaphore_wait(barrier, count - 1)

    def send(offset, carry):
        pltpu.make_async_remote_copy(
            src_ref=top_ref,
            dst_ref=tops.at[offset - 1],
            send_sem=top_send,
            recv_sem=top_recv,
            device_id=peer(offset),
            device_id_type=mesh,
        ).start()
        return carry

    lax.fori_loop(1, count, send, 0)
    copies = []
    for index, (target, move) in enumerate(((low, 1), (high, domains - 1))):
        side = pltpu.make_async_remote_copy(
            src_ref=block_ref,
            dst_ref=target,
            send_sem=side_send.at[index],
            recv_sem=side_recv.at[index],
            device_id={"dom": lax.rem(domain + move, domains), "sub": sub},
            device_id_type=mesh,
        )
        side.start()
        copies.append(side)
    arrived = tops.at[pl.ds(0, count - 1)]
    pltpu.make_async_copy(arrived, arrived, top_recv).wait()

    def gather(offset, carry):
        source = lax.rem(flat + count - offset, count) // subs
        slot = lax.rem(offset + count - 1, count)
        for r in range(top_cells):
            at = pl.ds(source * top_cells + r, 1)
            tops_out[at, :] = tops_out[at, :] + tops[slot, r : r + 1, :]
        return carry

    lax.fori_loop(0, count, gather, 0)
    for side in copies:
        side.wait()
    wide_out[:coeffs, :cells] = low[...]
    wide_out[:coeffs, 2 * cells :] = high[...]
    pltpu.make_async_copy(arrived, arrived, top_send).wait()


def exchange(block, partial, upward_ops, fine_list, mid_list, top_list, upper_list, rows, depth, counts):
    domains, subs = lax.axis_size("dom"), lax.axis_size("sub")
    coeffs, cells = block.shape
    top_cells = top_list.shape[1]
    vmem = pl.BlockSpec(memory_space=pltpu.VMEM)
    return pl.pallas_call(
        functools.partial(exchange_kernel, domains, subs, counts),
        in_specs=[vmem] * 7,
        out_specs=[vmem] * 4,
        out_shape=[
            jax.ShapeDtypeStruct((rows, 3 * cells), jnp.float32),
            jax.ShapeDtypeStruct((round_up(counts[4], LANES), 2 * LANES), jnp.float32),
            jax.ShapeDtypeStruct((depth, LANES), jnp.int32),
            jax.ShapeDtypeStruct((depth, LANES), jnp.int32),
        ],
        scratch_shapes=[
            pltpu.VMEM(block.shape, jnp.float32),
            pltpu.VMEM(block.shape, jnp.float32),
            pltpu.VMEM((domains * subs, top_cells, 2 * LANES), jnp.float32),
            pltpu.VMEM((top_cells, 2 * LANES), jnp.float32),
            pltpu.VMEM((rows, 8, 2 * LANES), jnp.float32),
            pltpu.VMEM((LANES, LANES), jnp.float32),
            pltpu.SemaphoreType.DMA((2,)),
            pltpu.SemaphoreType.DMA((2,)),
            pltpu.SemaphoreType.DMA,
            pltpu.SemaphoreType.DMA,
        ],
        compiler_params=pltpu.CompilerParams(
            collective_id=0, has_side_effects=True, vmem_limit_bytes=32 * 1024 * 1024
        ),
    )(
        block,
        partial,
        jnp.transpose(upward_ops, (1, 0, 2)),
        fine_list,
        jnp.transpose(mid_list),
        jnp.transpose(top_list),
        jnp.transpose(upper_list),
    )


def downward(expansions, downward_ops):
    spread = jnp.einsum("oab,bp->apo", downward_ops, expansions, precision=precise)
    return spread.reshape(spread.shape[0], -1)


def settle(portion):
    count = lax.axis_size("sub")
    ring = [(i, (i + 1) % count) for i in range(count)]
    total = moving = portion
    for _ in range(count - 1):
        moving = lax.ppermute(moving, "sub", ring)
        total = total + moving
    return total


def shards(
    fine_partial,
    upward_ops,
    interaction_ops,
    downward_ops,
    fine_list,
    mid_list,
    top_list,
    upper_list,
    positions,
    leaf_cell,
):
    slab_cells = fine_partial.shape[2]
    mid_cells = slab_cells // 8
    top_cells = slab_cells // 64
    domain = lax.axis_index("dom")
    slots, coeffs = interaction_ops.shape[:2]
    rows = round_up(coeffs, 24)
    depth = round_up(slots, 16)
    upper_span = max(1, top_cells // 8)
    spread = 3 * mid_cells
    tops = top_cells * lax.axis_size("dom")
    coarse_width = round_up(spread + tops + tops // 8, LANES)
    counts = (slab_cells, mid_cells, top_cells, spread, tops)
    partial = fine_partial[0]
    wide_fine, top_moments, fine_sources, coarse_sources = exchange(
        settle(partial), partial, upward_ops, fine_list, mid_list, top_list, upper_list,
        rows, depth, counts,
    )

    def padded(array, height, width, fill):
        return jnp.pad(
            array,
            ((0, height - array.shape[0]), (0, width - array.shape[1])),
            constant_values=fill,
        )

    terms = interact(
        wide_fine, top_moments, upward_ops, fine_sources, coarse_sources,
        jnp.transpose(interaction_ops, (1, 2, 0)), spread, tops, coarse_width,
    )
    terms = settle(terms)[:coeffs]
    at = LANES
    mid_term = terms[:, at : at + mid_cells]
    at += mid_cells
    top_term = terms[:, at : at + top_cells]
    at += top_cells
    local_upper = terms[:, at : at + upper_span]
    down_top = downward(local_upper, downward_ops)
    top_offset = domain * top_cells % 8
    local_top = top_term + lax.dynamic_slice_in_dim(down_top, top_offset, top_cells, 1)
    local_mid = mid_term + downward(local_top, downward_ops)
    local_fine = terms[:, :slab_cells] + downward(local_mid, downward_ops)
    potential = evaluate(
        padded(local_fine, rows, slab_cells, 0), leaf_cell - domain * slab_cells, positions
    )
    return (local_fine, potential)


def solution(mesh):
    placed = (
        P("sub", None, "dom"),
        P(),
        P("sub", None, None),
        P(),
        P("sub", "dom"),
        P("sub", "dom"),
        P("sub", "dom"),
        P("sub", None),
        P(None, ("dom", "sub")),
        P(("dom", "sub")),
    )
    return jax.shard_map(
        shards,
        mesh=mesh,
        in_specs=placed,
        out_specs=(P(None, "dom"), P(("dom", "sub"))),
        check_vma=False,
    )
```

```python
import functools

import jax
import jax.numpy as jnp
from jax import lax
from jax.experimental import pallas as pl
from jax.experimental.pallas import tpu as pltpu
from jax.sharding import PartitionSpec as P

ORDER = 8
LANES = 128


def round_up(count, unit):
    return -(-count // unit) * unit


def exponents():
    entries = []
    for degree in range(ORDER + 1):
        for along_x in range(degree, -1, -1):
            for along_y in range(degree - along_x, -1, -1):
                entries.append((along_x, along_y, degree - along_x - along_y))
    return entries


def halves(value):
    high = value.astype(jnp.bfloat16)
    low = (value - high.astype(jnp.float32)).astype(jnp.bfloat16)
    return high, low


def one_hot(row, count):
    places = lax.broadcasted_iota(jnp.int32, (count, row.shape[1]), 0)
    return jnp.where(places == row, 1.0, 0.0).astype(jnp.bfloat16)


def matmul(left, right):
    return jnp.dot(left, right, preferred_element_type=jnp.float32)


def one_hot_blocks(row, blocks):
    places = lax.broadcasted_iota(jnp.int32, (LANES, LANES), 0)
    places = places.astype(jnp.float32).astype(jnp.bfloat16)
    pieces = []
    for m in range(blocks):
        wanted = jnp.broadcast_to(row - float(LANES * m), (LANES, LANES)).astype(jnp.bfloat16)
        one, zero = jnp.ones((), jnp.bfloat16), jnp.zeros((), jnp.bfloat16)
        pieces.append(jnp.where(places == wanted, one, zero))
    return jnp.concatenate(pieces, axis=0)


def operator_copy(ops_ref, stage, arrived, part):
    coeffs = ops_ref.shape[0]
    count = min(8, coeffs - 8 * part)
    return pltpu.make_async_copy(
        ops_ref.at[:, pl.ds(8 * part, count), :],
        stage.at[part, :, pl.ds(0, count), :],
        arrived.at[part],
    )


def raise_level(moments, ops_high, ops_low):
    rows, width = moments.shape
    parents = round_up(width // 8, LANES)
    high, low = halves(moments)
    source = lax.broadcasted_iota(jnp.int32, (width, 8 * parents), 0)
    target = lax.broadcasted_iota(jnp.int32, (width, 8 * parents), 1)
    wanted = 8 * (target % parents) + target // parents
    chosen = jnp.where(source == wanted, 1.0, 0.0).astype(jnp.bfloat16)
    both = matmul(jnp.concatenate([high, low], axis=0), chosen)
    filler = jnp.zeros((2 * LANES - rows, parents), jnp.float32)
    stacks = []
    for first in (0, rows):
        pieces = []
        for o in range(8):
            pieces += [both[first : first + rows, o * parents : (o + 1) * parents], filler]
        stacks.append(jnp.concatenate(pieces, axis=0).astype(jnp.bfloat16))
    value = matmul(ops_high[...], stacks[0]) + matmul(ops_high[...], stacks[1])
    return value + matmul(ops_low[...], stacks[0])


def transfer(source, target, sems, index, place):
    return pltpu.make_async_remote_copy(
        src_ref=source,
        dst_ref=target,
        send_sem=sems[0].at[index],
        recv_sem=sems[1].at[index],
        device_id=place,
        device_id_type=pl.DeviceIdType.MESH,
    )


def total_of(first, others):
    for k in range(others.shape[0]):
        first = first + others[k]
    return first


def padded(value, height, width):
    below, beside = height - value.shape[0], width - value.shape[1]
    if beside:
        filler = jnp.zeros((value.shape[0], beside), value.dtype)
        value = jnp.concatenate([value, filler], axis=1)
    if below:
        value = jnp.concatenate([value, jnp.zeros((below, width), value.dtype)], axis=0)
    return value


def fill_octant(ops, octant, high_ref, low_ref):
    coeffs = ops.shape[1]
    at = 2 * LANES * octant
    high_ref[:coeffs, at : at + coeffs], low_ref[:coeffs, at : at + coeffs] = halves(ops[octant])


def spread_level(expansions, offset, ops_high, ops_low):
    rows = expansions.shape[0]
    parent = lax.broadcasted_iota(jnp.int32, (LANES, LANES), 0)
    child = lax.broadcasted_iota(jnp.int32, (LANES, LANES), 1) + offset
    copied = jnp.where(child // 8 == parent, 1.0, 0.0).astype(jnp.bfloat16)
    high, low = halves(expansions)
    both = matmul(jnp.concatenate([high, low], axis=0), copied).astype(jnp.bfloat16)
    wide = jnp.concatenate([both[:rows], both[rows:]], axis=1).astype(jnp.float32)
    wide = padded(wide, 2 * LANES, 2 * LANES)
    octant = (lax.broadcasted_iota(jnp.int32, wide.shape, 1) % LANES + offset) % 8
    pieces = [jnp.where(octant == o, wide, 0.0).astype(jnp.bfloat16) for o in range(8)]
    right = jnp.concatenate(pieces, axis=0)
    first = matmul(ops_high[...], right)
    second = matmul(ops_low[...], right[:, :LANES])
    return first[:, :LANES] + first[:, LANES:] + second


def pick_slots(lists, which, table, picked, rows, blocks):
    depth = lists.shape[1]
    stride = picked.shape[0] // (rows + 1)
    batch = 32 if depth % 32 == 0 else 16

    def step(number, carry):
        base = pl.multiple_of(number * batch, batch)
        for slot in range(0, batch, 2):
            pair = [
                one_hot_blocks(lists[which, pl.ds(base + slot + m, 1), :], blocks)
                for m in range(2)
            ]
            chosen = jnp.concatenate(pair, axis=1)
            if which:
                value = matmul(table[...], jnp.concatenate([chosen, chosen], axis=0))
            else:
                near, far = chosen[: 2 * LANES], chosen[2 * LANES :]
                value = matmul(table[0], near) + matmul(table[1], near)
                value += matmul(table[2], jnp.concatenate([far, far], axis=0))
            for m in range(2):
                at = pl.ds(base + slot + m, rows, stride)
                picked[at, :] = value[:, m * LANES : (m + 1) * LANES]
        return carry

    lax.fori_loop(0, depth // batch, step, 0)


def contract(stage, fine_picked, coarse_picked, rows, depth):
    coeffs, slots = stage.shape[1], stage.shape[3]
    stride = fine_picked.shape[0] // (rows + 1)
    below = jnp.zeros((LANES - depth, 2 * LANES), jnp.bfloat16)
    total = None
    for first in range(0, coeffs, 24):
        left = []
        right = []
        for term in range(first, min(first + 24, coeffs)):
            block = stage.at[term // 8].reshape(coeffs * 8, slots)
            op_high, op_low = halves(padded(block[pl.ds(term % 8, coeffs, 8), :], rows, LANES))
            place = pl.ds(term * stride, depth)
            data = jnp.concatenate([fine_picked[place, :], coarse_picked[place, :]], axis=1)
            high, low = halves(data)
            high = jnp.concatenate([high, below], axis=0)
            low = jnp.concatenate([low, below], axis=0)
            left += [op_high, op_high, op_low]
            right += [high, low, high]
        product = matmul(jnp.concatenate(left, axis=1), jnp.concatenate(right, axis=0))
        total = product if total is None else total + product
    return total


def step_kernel(
    domains, subs, counts, partial_ref, upward_ref, ops_ref, downward_ref, fine_ref, mid_ref,
    top_list_ref, upper_ref, leaf_ref, position_ref, exponent_ref,
    local_out, potential_out,
    mine, upward, downward, fine_in, mid_in, top_in, upper_in, leaves, positions, powers,
    stage, up_high, up_low, down_high, down_low, mids, top_ref, parts, mid_parts, sums,
    mid_sums, low, high, mid_rows, tops, top_rows, lists, turned_lists, fine_table,
    coarse_table, fine_picked, coarse_picked, fine_terms, coarse_terms, fine_parts,
    coarse_parts, chosen_ref, factors_ref,
    load, arrived_ops, part_send, part_recv, side_send, side_recv, top_send, top_recv,
    term_send, term_recv,
):
    domain, sub = lax.axis_index("dom"), lax.axis_index("sub")
    slab, mid, top, spread, all_tops = counts
    count = domains * subs
    flat = domain * subs + sub
    coeffs, cells = mine.shape
    rows = up_high.shape[0]
    depth = lists.shape[1]
    slots = fine_in.shape[0]
    particles = leaves.shape[1]
    width = coarse_table.shape[1] // 2
    part_sems, side_sems = (part_send, part_recv), (side_send, side_recv)
    term_sems = (term_send, term_recv)

    loads = [pltpu.make_async_copy(partial_ref.at[:, 0, :], mine, load.at[0])]
    for o in range(8):
        loads.append(
            pltpu.make_async_copy(upward_ref.at[:, o, :], upward.at[o], load.at[1 + o])
        )
    for k, (source, target) in enumerate(
        (
            (fine_ref, fine_in), (mid_ref, mid_in), (top_list_ref, top_in),
            (upper_ref, upper_in), (leaf_ref, leaves), (position_ref, positions),
            (exponent_ref, powers),
        )
    ):
        loads.append(pltpu.make_async_copy(source, target, load.at[9 + k]))
    downs = [
        pltpu.make_async_copy(downward_ref.at[:, o, :], downward.at[o], load.at[16 + o])
        for o in range(8)
    ]
    for one in loads:
        one.start()
    barrier = pltpu.get_barrier_semaphore()

    def peer(offset):
        place = lax.rem(flat + offset, count)
        return {"dom": place // subs, "sub": lax.rem(place, subs)}

    def greet(offset, carry):
        pl.semaphore_signal(
            barrier, inc=1, device_id=peer(offset), device_id_type=pl.DeviceIdType.MESH
        )
        return carry

    mid_rows[...] = jnp.zeros_like(mid_rows)
    top_rows[...] = jnp.zeros_like(top_rows)
    lax.fori_loop(1, count, greet, 0)
    for ref in (up_high, up_low, down_high, down_low):
        ref[...] = jnp.zeros_like(ref)
    for o in range(8):
        loads[1 + o].wait()
        fill_octant(upward, o, up_high, up_low)
    loads[0].wait()
    for one in downs:
        one.start()
    for part in range(stage.shape[0]):
        operator_copy(ops_ref, stage, arrived_ops, part).start()
    mid_moments = raise_level(padded(mine[...], rows, cells), up_high, up_low)
    top_moments = raise_level(mid_moments, up_high, up_low)
    both = mid_moments + pltpu.roll(top_moments, mid, 1)
    turned = jnp.transpose(padded(both, 2 * LANES, LANES))
    mids[...] = turned[:mid]
    top_ref[...] = turned[mid : mid + top]
    tops[count - 1] = top_ref[...]
    pl.semaphore_wait(barrier, count - 1)

    def send(offset, carry):
        pltpu.make_async_remote_copy(
            src_ref=top_ref,
            dst_ref=tops.at[offset - 1],
            send_sem=top_send,
            recv_sem=top_recv,
            device_id=peer(offset),
            device_id_type=pl.DeviceIdType.MESH,
        ).start()
        return carry

    lax.fori_loop(1, count, send, 0)
    sub_peers = [{"dom": domain, "sub": lax.rem(sub + k + 1, subs)} for k in range(subs - 1)]
    copies = []
    for k, place in enumerate(sub_peers):
        copies.append(transfer(mine, parts.at[k], part_sems, 2 * k, place))
        copies.append(transfer(mids, mid_parts.at[k], part_sems, 2 * k + 1, place))
    for one in copies:
        one.start()

    for one in loads[9:]:
        one.wait()

    def place_in(sources, offset):
        return jnp.where(sources >= 0, sources + offset, -1).astype(jnp.float32)

    lists[0, :slots] = place_in(fine_in[...], slab - domain * slab)
    lists[0, slots:] = jnp.full((depth - slots, LANES), -1.0, jnp.float32)
    turned_lists[...] = jnp.full_like(turned_lists, -1.0)
    start = 0
    for part in (
        place_in(mid_in[...], mid - domain * mid),
        place_in(top_in[...], spread),
        place_in(upper_in[pl.ds(domain * top // 8, 1), :], spread + all_tops),
    ):
        turned_lists[start : start + part.shape[0], :slots] = part
        start += part.shape[0]
    lists[1] = jnp.transpose(turned_lists[...])[:depth]

    for one in copies:
        one.wait()
    sums[...] = total_of(mine[...], parts)
    mid_sums[...] = total_of(mids[...], mid_parts)
    copies = []
    for index, (target, first, move) in enumerate(((low, 0, 1), (high, 2 * mid, domains - 1))):
        place = {"dom": lax.rem(domain + move, domains), "sub": sub}
        copies.append(transfer(sums, target, side_sems, 2 * index, place))
        rows_there = mid_rows.at[pl.ds(first, mid)]
        copies.append(transfer(mid_sums, rows_there, side_sems, 2 * index + 1, place))
    for one in copies:
        one.start()

    def split(block):
        return halves(padded(block, rows, LANES))

    fine_table[0, :, LANES:], fine_table[1, :, LANES:] = split(sums[...])
    for o in range(8):
        downs[o].wait()
        fill_octant(downward, o, down_high, down_low)
    masks = [
        [(powers[:, axis : axis + 1] // bit) % 2 == 1 for bit in (1, 2, 4, 8)]
        for axis in range(3)
    ]

    def factor(number, carry):
        span = pl.ds(pl.multiple_of(number * LANES, LANES), LANES)
        chosen_ref[:, span] = one_hot(leaves[:, span] - domain * slab, cells)
        value = jnp.ones((rows, LANES), jnp.float32)
        for axis in range(3):
            power = positions[axis : axis + 1, span]
            for bit in range(4):
                value = value * jnp.where(masks[axis][bit], power, 1.0)
                power = power * power
        factors_ref[:, span] = value
        return carry

    lax.fori_loop(0, particles // LANES, factor, 0)
    for one in copies:
        one.wait()
    fine_table[0, :, :LANES], fine_table[1, :, :LANES] = split(low[...])
    fine_table[2, :, :LANES], fine_table[2, :, LANES:] = split(high[...])
    pick_slots(lists, 0, fine_table, fine_picked, rows, 3)

    arrived = tops.at[pl.ds(0, count - 1)]
    pltpu.make_async_copy(arrived, arrived, top_recv).wait()

    def gather(offset, carry):
        source = lax.rem(flat + count - offset, count) // subs
        slot = lax.rem(offset + count - 1, count)
        for r in range(top):
            at = pl.ds(source * top + r, 1)
            top_rows[at, :] = top_rows[at, :] + tops[slot, r : r + 1, :]
        return carry

    lax.fori_loop(0, count, gather, 0)

    def shifted(value, amount):
        value = padded(value, rows, width)
        return pltpu.roll(value, amount, 1) if amount else value

    mid_rows[mid : 2 * mid] = mid_sums[...]
    top_moments = jnp.transpose(top_rows[...])[:rows]
    coarse = shifted(top_moments, spread)
    coarse += shifted(raise_level(top_moments, up_high, up_low), spread + all_tops)
    coarse += shifted(jnp.transpose(mid_rows[...])[:rows], 0)
    coarse_table[:, :width], coarse_table[:, width:] = halves(coarse)
    pick_slots(lists, 1, coarse_table, coarse_picked, rows, width // LANES)

    for part in range(stage.shape[0]):
        operator_copy(ops_ref, stage, arrived_ops, part).wait()
    total = contract(stage, fine_picked, coarse_picked, rows, depth)
    fine_terms[...] = total[:, :LANES]
    turned = jnp.transpose(padded(total[:, LANES:], 2 * LANES, LANES))
    coarse_terms[...] = turned[: coarse_terms.shape[0]]
    coarse_copies = []
    fine_copies = []
    for k, place in enumerate(sub_peers):
        coarse_copies.append(
            transfer(coarse_terms, coarse_parts.at[k], term_sems, 2 * k, place)
        )
        fine_copies.append(transfer(fine_terms, fine_parts.at[k], term_sems, 2 * k + 1, place))
    for one in coarse_copies + fine_copies:
        one.start()
    for one in coarse_copies:
        one.wait()
    coarse = jnp.transpose(padded(total_of(coarse_terms[...], coarse_parts), LANES, 2 * LANES))
    coarse = coarse[:rows]
    lane = lax.broadcasted_iota(jnp.int32, coarse.shape, 1)

    def columns(first, number):
        value = pltpu.roll(coarse, LANES - first, 1) if first else coarse
        return jnp.where(lane < number, value, 0.0)

    local = columns(mid + top, 1)
    local = columns(mid, top) + spread_level(local, domain * top % 8, down_high, down_low)
    local = jnp.where(lane < top, local, 0.0)
    local = columns(0, mid) + spread_level(local, 0, down_high, down_low)
    local = spread_level(local, 0, down_high, down_low)
    for one in fine_copies:
        one.wait()
    local = total_of(fine_terms[...], fine_parts) + local
    local_out[...] = local[:coeffs]
    table = jnp.concatenate(halves(local), axis=1)
    for start in range(0, particles, 2 * LANES):
        span = slice(start, start + 2 * LANES)
        chosen = chosen_ref[:, span]
        value = matmul(table, jnp.concatenate([chosen, chosen], axis=0)) * factors_ref[:, span]
        potential_out[:, span] = jnp.sum(value, axis=0, keepdims=True)
    pltpu.make_async_copy(arrived, arrived, top_send).wait()


def shards(
    fine_partial,
    upward_ops,
    interaction_ops,
    downward_ops,
    fine_list,
    mid_list,
    top_list,
    upper_list,
    positions,
    leaf_cell,
):
    domains, subs = lax.axis_size("dom"), lax.axis_size("sub")
    slab = fine_partial.shape[2]
    mid = slab // 8
    top = slab // 64
    slots, coeffs = interaction_ops.shape[:2]
    particles = leaf_cell.shape[0]
    rows = round_up(coeffs, 24)
    depth = round_up(slots, 16)
    parts = round_up(coeffs, 8) // 8
    picked = (rows + 1) * (depth + 8)
    spread = 3 * mid
    tops = top * domains
    coarse_rows = round_up(mid + top + 1, 8)
    counts = (slab, mid, top, spread, tops)
    width = round_up(spread + tops + tops // 8, LANES)
    others = max(subs - 1, 1)
    wide = 2 * LANES
    f32, bf16, i32 = jnp.float32, jnp.bfloat16, jnp.int32
    table = jnp.asarray(exponents(), i32)
    table = jnp.pad(table, ((0, rows - coeffs), (0, LANES - 3)))
    shapes = [
        ((coeffs, slab), f32),
        ((8, coeffs, coeffs), f32),
        ((8, coeffs, coeffs), f32),
        ((slots, slab), i32),
        ((mid, slots), i32),
        ((top, slots), i32),
        ((upper_list.shape[1], slots), i32),
        ((1, particles), i32),
        ((3, particles), f32),
        ((rows, LANES), i32),
        ((parts, coeffs, 8, slots), f32),
        ((rows, 8 * wide), bf16),
        ((rows, 8 * wide), bf16),
        ((rows, 8 * wide), bf16),
        ((rows, 8 * wide), bf16),
        ((mid, wide), f32),
        ((top, wide), f32),
        ((others, coeffs, slab), f32),
        ((others, mid, wide), f32),
        ((coeffs, slab), f32),
        ((mid, wide), f32),
        ((coeffs, slab), f32),
        ((coeffs, slab), f32),
        ((LANES, wide), f32),
        ((domains * subs, top, wide), f32),
        ((round_up(tops, LANES), wide), f32),
        ((2, depth, LANES), f32),
        ((LANES, LANES), f32),
        ((3, rows, wide), bf16),
        ((rows, 2 * width), bf16),
        ((picked, LANES), f32),
        ((picked, LANES), f32),
        ((rows, LANES), f32),
        ((coarse_rows, wide), f32),
        ((others, rows, LANES), f32),
        ((others, coarse_rows, wide), f32),
        ((slab, particles), bf16),
        ((rows, particles), f32),
    ]
    semaphores = [(24,), (parts,)] + 2 * [(2 * others,)] + 2 * [(4,)] + 2 * [()]
    semaphores += 2 * [(2 * others,)]
    vmem = pl.BlockSpec(memory_space=pltpu.VMEM)
    local_fine, potential = pl.pallas_call(
        functools.partial(step_kernel, domains, subs, counts),
        in_specs=[pl.BlockSpec(memory_space=pltpu.HBM)] * 11,
        out_specs=[vmem] * 2,
        out_shape=[
            jax.ShapeDtypeStruct((coeffs, slab), f32),
            jax.ShapeDtypeStruct((1, particles), f32),
        ],
        scratch_shapes=[pltpu.VMEM(*one) for one in shapes]
        + [pltpu.SemaphoreType.DMA(one) if one else pltpu.SemaphoreType.DMA for one in semaphores],
        compiler_params=pltpu.CompilerParams(
            collective_id=0, has_side_effects=True, vmem_limit_bytes=67_043_328
        ),
    )(
        jnp.transpose(fine_partial, (1, 0, 2)),
        jnp.transpose(upward_ops, (1, 0, 2)),
        jnp.transpose(interaction_ops, (1, 2, 0)),
        jnp.transpose(downward_ops, (1, 0, 2)),
        fine_list,
        jnp.transpose(mid_list),
        jnp.transpose(top_list),
        jnp.transpose(upper_list),
        leaf_cell[None],
        positions,
        table,
    )
    return local_fine, potential[0]


def solution(mesh):
    placed = (
        P("sub", None, "dom"),
        P(),
        P("sub", None, None),
        P(),
        P("sub", "dom"),
        P("sub", "dom"),
        P("sub", "dom"),
        P("sub", None),
        P(None, ("dom", "sub")),
        P(("dom", "sub")),
    )
    return jax.shard_map(
        shards,
        mesh=mesh,
        in_specs=placed,
        out_specs=(P(None, "dom"), P(("dom", "sub"))),
        check_vma=False,
    )
```

```python
import functools

import jax
import jax.numpy as jnp
from jax import lax
from jax.experimental import pallas as pl
from jax.experimental.pallas import tpu as pltpu
from jax.sharding import PartitionSpec as P

ORDER = 8
LANES = 128


def round_up(count, unit):
    return -(-count // unit) * unit


def exponents():
    entries = []
    for degree in range(ORDER + 1):
        for along_x in range(degree, -1, -1):
            for along_y in range(degree - along_x, -1, -1):
                entries.append((along_x, along_y, degree - along_x - along_y))
    return entries


def halves(value):
    high = value.astype(jnp.bfloat16)
    low = (value - high.astype(jnp.float32)).astype(jnp.bfloat16)
    return high, low


def one_hot(row, count):
    places = lax.broadcasted_iota(jnp.int32, (count, row.shape[1]), 0)
    return jnp.where(places == row, 1.0, 0.0).astype(jnp.bfloat16)


def matmul(left, right):
    return jnp.dot(left, right, preferred_element_type=jnp.float32)


def one_hot_blocks(row, blocks):
    places = lax.broadcasted_iota(jnp.int32, (LANES, LANES), 0)
    places = places.astype(jnp.float32).astype(jnp.bfloat16)
    pieces = []
    for m in blocks:
        wanted = jnp.broadcast_to(row - float(LANES * m), (LANES, LANES)).astype(jnp.bfloat16)
        one, zero = jnp.ones((), jnp.bfloat16), jnp.zeros((), jnp.bfloat16)
        pieces.append(jnp.where(places == wanted, one, zero))
    return jnp.concatenate(pieces, axis=0)


def operator_copy(ops_ref, stage, arrived, part):
    coeffs = ops_ref.shape[0]
    count = min(8, coeffs - 8 * part)
    return pltpu.make_async_copy(
        ops_ref.at[:, pl.ds(8 * part, count), :],
        stage.at[part, :, pl.ds(0, count), :],
        arrived.at[part],
    )


def raise_level(moments, ops_high, ops_low):
    rows, width = moments.shape
    parents = round_up(width // 8, LANES)
    high, low = halves(moments)
    source = lax.broadcasted_iota(jnp.int32, (width, 8 * parents), 0)
    target = lax.broadcasted_iota(jnp.int32, (width, 8 * parents), 1)
    wanted = 8 * (target % parents) + target // parents
    chosen = jnp.where(source == wanted, 1.0, 0.0).astype(jnp.bfloat16)
    both = matmul(jnp.concatenate([high, low], axis=0), chosen)
    filler = jnp.zeros((2 * LANES - rows, parents), jnp.float32)
    stacks = []
    for first in (0, rows):
        pieces = []
        for o in range(8):
            pieces += [both[first : first + rows, o * parents : (o + 1) * parents], filler]
        stacks.append(jnp.concatenate(pieces, axis=0).astype(jnp.bfloat16))
    value = matmul(ops_high[...], stacks[0]) + matmul(ops_high[...], stacks[1])
    return value + matmul(ops_low[...], stacks[0])


def transfer(source, target, sems, index, place):
    return pltpu.make_async_remote_copy(
        src_ref=source,
        dst_ref=target,
        send_sem=sems[0].at[index],
        recv_sem=sems[1].at[index],
        device_id=place,
        device_id_type=pl.DeviceIdType.MESH,
    )


def total_of(first, others):
    for k in range(others.shape[0]):
        first = first + others[k]
    return first


def padded(value, height, width):
    below, beside = height - value.shape[0], width - value.shape[1]
    if beside:
        filler = jnp.zeros((value.shape[0], beside), value.dtype)
        value = jnp.concatenate([value, filler], axis=1)
    if below:
        value = jnp.concatenate([value, jnp.zeros((below, width), value.dtype)], axis=0)
    return value


def fill_octant(ops, octant, high_ref, low_ref):
    coeffs = ops.shape[1]
    at = 2 * LANES * octant
    high_ref[:coeffs, at : at + coeffs], low_ref[:coeffs, at : at + coeffs] = halves(ops[octant])


def spread_level(expansions, offset, ops_high, ops_low):
    rows = expansions.shape[0]
    parent = lax.broadcasted_iota(jnp.int32, (LANES, LANES), 0)
    child = lax.broadcasted_iota(jnp.int32, (LANES, LANES), 1) + offset
    copied = jnp.where(child // 8 == parent, 1.0, 0.0).astype(jnp.bfloat16)
    high, low = halves(expansions)
    both = matmul(jnp.concatenate([high, low], axis=0), copied).astype(jnp.bfloat16)
    wide = jnp.concatenate([both[:rows], both[rows:]], axis=1).astype(jnp.float32)
    wide = padded(wide, 2 * LANES, 2 * LANES)
    octant = (lax.broadcasted_iota(jnp.int32, wide.shape, 1) % LANES + offset) % 8
    pieces = [jnp.where(octant == o, wide, 0.0).astype(jnp.bfloat16) for o in range(8)]
    right = jnp.concatenate(pieces, axis=0)
    first = matmul(ops_high[...], right)
    second = matmul(ops_low[...], right[:, :LANES])
    return first[:, :LANES] + first[:, LANES:] + second


def pick_slots(list_ref, tables, picked, rows, blocks, repeats, adding):
    depth = list_ref.shape[0]
    stride = picked.shape[0] // (rows + 1)
    batch = 32 if depth % 32 == 0 else 16

    def step(number, carry):
        base = pl.multiple_of(number * batch, batch)
        for slot in range(0, batch, 2):
            pair = [
                one_hot_blocks(list_ref[pl.ds(base + slot + m, 1), :], blocks) for m in range(2)
            ]
            chosen = jnp.concatenate(pair, axis=1)
            chosen = jnp.concatenate([chosen] * repeats, axis=0)
            value = matmul(tables[0][...], chosen)
            for table in tables[1:]:
                value += matmul(table[...], chosen)
            for m in range(2):
                at = pl.ds(base + slot + m, rows, stride)
                part = value[:, m * LANES : (m + 1) * LANES]
                picked[at, :] = picked[at, :] + part if adding else part
        return carry

    lax.fori_loop(0, depth // batch, step, 0)


def contract(stage, fine_picked, coarse_picked, rows, depth):
    coeffs, slots = stage.shape[1], stage.shape[3]
    stride = fine_picked.shape[0] // (rows + 1)
    below = jnp.zeros((LANES - depth, 2 * LANES), jnp.bfloat16)
    total = None
    for first in range(0, coeffs, 24):
        left = []
        right = []
        for term in range(first, min(first + 24, coeffs)):
            block = stage.at[term // 8].reshape(coeffs * 8, slots)
            op_high, op_low = halves(padded(block[pl.ds(term % 8, coeffs, 8), :], rows, LANES))
            place = pl.ds(term * stride, depth)
            data = jnp.concatenate([fine_picked[place, :], coarse_picked[place, :]], axis=1)
            high, low = halves(data)
            high = jnp.concatenate([high, below], axis=0)
            low = jnp.concatenate([low, below], axis=0)
            left += [op_high, op_high, op_low]
            right += [high, low, high]
        product = matmul(jnp.concatenate(left, axis=1), jnp.concatenate(right, axis=0))
        total = product if total is None else total + product
    return total


def step_kernel(
    domains, subs, counts, partial_ref, upward_ref, ops_ref, downward_ref, fine_ref, mid_ref,
    top_list_ref, upper_ref, leaf_ref, position_ref, exponent_ref,
    local_out, potential_out,
    mine, upward, downward, fine_in, mid_in, top_in, upper_in, leaves, positions, powers,
    stage, up_high, up_low, down_high, down_low, mids, top_ref, parts, mid_parts, sums,
    mid_sums, low, high, mid_rows, tops, top_rows, lists, turned_lists, fine_table,
    coarse_table, fine_picked, coarse_picked, fine_terms, coarse_terms, fine_parts,
    coarse_parts, chosen_ref, factors_ref, coarse_ref,
    load, arrived_ops, part_send, part_recv, side_send, side_recv, top_send, top_recv,
    term_send, term_recv,
):
    domain, sub = lax.axis_index("dom"), lax.axis_index("sub")
    slab, mid, top, spread, all_tops = counts
    count = domains * subs
    flat = domain * subs + sub
    coeffs, cells = mine.shape
    rows = up_high.shape[0]
    depth = lists.shape[1]
    slots = fine_in.shape[0]
    particles = leaves.shape[1]
    width = coarse_table.shape[1] // 2
    part_sems, side_sems = (part_send, part_recv), (side_send, side_recv)
    term_sems = (term_send, term_recv)

    loads = [pltpu.make_async_copy(partial_ref.at[:, 0, :], mine, load.at[0])]
    for o in range(8):
        loads.append(
            pltpu.make_async_copy(upward_ref.at[:, o, :], upward.at[o], load.at[1 + o])
        )
    for k, (source, target) in enumerate(
        (
            (fine_ref, fine_in), (mid_ref, mid_in), (top_list_ref, top_in),
            (upper_ref, upper_in), (leaf_ref, leaves), (position_ref, positions),
            (exponent_ref, powers),
        )
    ):
        loads.append(pltpu.make_async_copy(source, target, load.at[9 + k]))
    downs = [
        pltpu.make_async_copy(downward_ref.at[:, o, :], downward.at[o], load.at[16 + o])
        for o in range(8)
    ]
    for one in loads:
        one.start()
    barrier = pltpu.get_barrier_semaphore()

    def peer(offset):
        place = lax.rem(flat + offset, count)
        return {"dom": place // subs, "sub": lax.rem(place, subs)}

    def greet(offset, carry):
        pl.semaphore_signal(
            barrier, inc=1, device_id=peer(offset), device_id_type=pl.DeviceIdType.MESH
        )
        return carry

    mid_rows[...] = jnp.zeros_like(mid_rows)
    top_rows[...] = jnp.zeros_like(top_rows)
    lax.fori_loop(1, count, greet, 0)
    for ref in (up_high, up_low, down_high, down_low):
        ref[...] = jnp.zeros_like(ref)
    for o in range(8):
        loads[1 + o].wait()
        fill_octant(upward, o, up_high, up_low)
    loads[0].wait()
    for one in downs:
        one.start()
    for part in range(stage.shape[0]):
        operator_copy(ops_ref, stage, arrived_ops, part).start()
    mid_moments = raise_level(padded(mine[...], rows, cells), up_high, up_low)
    top_moments = raise_level(mid_moments, up_high, up_low)
    both = mid_moments + pltpu.roll(top_moments, mid, 1)
    turned = jnp.transpose(padded(both, 2 * LANES, LANES))
    mids[...] = turned[:mid]
    top_ref[...] = turned[mid : mid + top]
    tops[count - 1] = top_ref[...]
    pl.semaphore_wait(barrier, count - 1)

    def send(offset, carry):
        pltpu.make_async_remote_copy(
            src_ref=top_ref,
            dst_ref=tops.at[offset - 1],
            send_sem=top_send,
            recv_sem=top_recv,
            device_id=peer(offset),
            device_id_type=pl.DeviceIdType.MESH,
        ).start()
        return carry

    lax.fori_loop(1, count, send, 0)
    sub_peers = [{"dom": domain, "sub": lax.rem(sub + k + 1, subs)} for k in range(subs - 1)]
    copies = []
    for k, place in enumerate(sub_peers):
        copies.append(transfer(mine, parts.at[k], part_sems, 2 * k, place))
        copies.append(transfer(mids, mid_parts.at[k], part_sems, 2 * k + 1, place))
    for one in copies:
        one.start()

    for one in loads[9:]:
        one.wait()

    def place_in(sources, offset):
        return jnp.where(sources >= 0, sources + offset, -1).astype(jnp.float32)

    lists[0, :slots] = place_in(fine_in[...], slab - domain * slab)
    lists[0, slots:] = jnp.full((depth - slots, LANES), -1.0, jnp.float32)
    turned_lists[...] = jnp.full_like(turned_lists, -1.0)
    start = 0
    for part in (
        place_in(mid_in[...], mid - domain * mid),
        place_in(top_in[...], spread),
        place_in(upper_in[pl.ds(domain * top // 8, 1), :], spread + all_tops),
    ):
        turned_lists[start : start + part.shape[0], :slots] = part
        start += part.shape[0]
    lists[1] = jnp.transpose(turned_lists[...])[:depth]

    lane = lax.broadcasted_iota(jnp.int32, (rows, LANES), 1)
    takes = []
    for axis in range(3):
        taken = (lane < 48) & (lane % 16 == powers[:, axis : axis + 1])
        takes.append(jnp.where(taken, 1.0, 0.0).astype(jnp.bfloat16))
    power = lax.broadcasted_iota(jnp.int32, (16, 2 * LANES), 0)
    power_bits = [(power // bit) % 2 == 1 for bit in (1, 2, 4, 8)]
    below = jnp.zeros((LANES - 48, 2 * LANES), jnp.bfloat16)

    def factor(number, carry):
        span = pl.ds(pl.multiple_of(number * 2 * LANES, 2 * LANES), 2 * LANES)
        chosen_ref[:, span] = one_hot(leaves[:, span] - domain * slab, cells)
        value = None
        for axis in range(3):
            base = positions[axis : axis + 1, span]
            raised = jnp.ones((16, 2 * LANES), jnp.float32)
            for bit in power_bits:
                raised = raised * jnp.where(bit, base, 1.0)
                base = base * base
            first, rest = halves(raised)
            left_over = raised - first.astype(jnp.float32) - rest.astype(jnp.float32)
            stack = jnp.concatenate(
                [first, rest, left_over.astype(jnp.bfloat16), below], axis=0
            )
            taken = matmul(takes[axis], stack)
            value = taken if value is None else value * taken
        factors_ref[:, span] = value
        return carry

    lax.fori_loop(0, particles // (2 * LANES), factor, 0)
    for o in range(8):
        downs[o].wait()
        fill_octant(downward, o, down_high, down_low)
    for one in copies:
        one.wait()
    sums[...] = total_of(mine[...], parts)
    mid_sums[...] = total_of(mids[...], mid_parts)
    copies = []
    for index, (target, first, move) in enumerate(((low, 0, 1), (high, 2 * mid, domains - 1))):
        place = {"dom": lax.rem(domain + move, domains), "sub": sub}
        copies.append(transfer(sums, target, side_sems, 2 * index, place))
        rows_there = mid_rows.at[pl.ds(first, mid)]
        copies.append(transfer(mid_sums, rows_there, side_sems, 2 * index + 1, place))
    for one in copies:
        one.start()

    def split(block):
        return halves(padded(block, rows, LANES))

    fine_table[0, :, :LANES], fine_table[0, :, LANES:] = split(sums[...])
    pick_slots(lists.at[0], [fine_table.at[0]], fine_picked, rows, (1,), 2, False)
    arrived = tops.at[pl.ds(0, count - 1)]
    pltpu.make_async_copy(arrived, arrived, top_recv).wait()

    def gather(offset, carry):
        source = lax.rem(flat + count - offset, count) // subs
        slot = lax.rem(offset + count - 1, count)
        for r in range(top):
            at = pl.ds(source * top + r, 1)
            top_rows[at, :] = top_rows[at, :] + tops[slot, r : r + 1, :]
        return carry

    lax.fori_loop(0, count, gather, 0)

    def shifted(value, amount):
        value = padded(value, rows, width)
        return pltpu.roll(value, amount, 1) if amount else value

    top_moments = jnp.transpose(top_rows[...])[:rows]
    coarse = shifted(top_moments, spread)
    coarse += shifted(raise_level(top_moments, up_high, up_low), spread + all_tops)
    coarse_ref[...] = coarse
    for one in copies:
        one.wait()
    fine_table[1, :, :LANES], fine_table[2, :, :LANES] = split(low[...])
    fine_table[1, :, LANES:], fine_table[2, :, LANES:] = split(high[...])
    sides = [fine_table.at[1], fine_table.at[2]]
    pick_slots(lists.at[0], sides, fine_picked, rows, (0, 2), 1, True)

    mid_rows[mid : 2 * mid] = mid_sums[...]
    coarse = coarse_ref[...] + shifted(jnp.transpose(mid_rows[...])[:rows], 0)
    coarse_table[:, :width], coarse_table[:, width:] = halves(coarse)
    blocks = tuple(range(width // LANES))
    pick_slots(lists.at[1], [coarse_table], coarse_picked, rows, blocks, 2, False)

    for part in range(stage.shape[0]):
        operator_copy(ops_ref, stage, arrived_ops, part).wait()
    total = contract(stage, fine_picked, coarse_picked, rows, depth)
    fine_terms[...] = total[:, :LANES]
    turned = jnp.transpose(padded(total[:, LANES:], 2 * LANES, LANES))
    coarse_terms[...] = turned[: coarse_terms.shape[0]]
    coarse_copies = []
    fine_copies = []
    for k, place in enumerate(sub_peers):
        coarse_copies.append(
            transfer(coarse_terms, coarse_parts.at[k], term_sems, 2 * k, place)
        )
        fine_copies.append(transfer(fine_terms, fine_parts.at[k], term_sems, 2 * k + 1, place))
    for one in coarse_copies + fine_copies:
        one.start()
    for one in coarse_copies:
        one.wait()
    coarse = jnp.transpose(padded(total_of(coarse_terms[...], coarse_parts), LANES, 2 * LANES))
    coarse = coarse[:rows]
    lane = lax.broadcasted_iota(jnp.int32, coarse.shape, 1)

    def columns(first, number):
        value = pltpu.roll(coarse, LANES - first, 1) if first else coarse
        return jnp.where(lane < number, value, 0.0)

    local = columns(mid + top, 1)
    local = columns(mid, top) + spread_level(local, domain * top % 8, down_high, down_low)
    local = jnp.where(lane < top, local, 0.0)
    local = columns(0, mid) + spread_level(local, 0, down_high, down_low)
    local = spread_level(local, 0, down_high, down_low)
    for one in fine_copies:
        one.wait()
    local = total_of(fine_terms[...], fine_parts) + local
    local_out[...] = local[:coeffs]
    table = jnp.concatenate(halves(local), axis=1)
    for start in range(0, particles, 2 * LANES):
        span = slice(start, start + 2 * LANES)
        chosen = chosen_ref[:, span]
        value = matmul(table, jnp.concatenate([chosen, chosen], axis=0)) * factors_ref[:, span]
        potential_out[:, span] = jnp.sum(value, axis=0, keepdims=True)
    pltpu.make_async_copy(arrived, arrived, top_send).wait()


def shards(
    fine_partial,
    upward_ops,
    interaction_ops,
    downward_ops,
    fine_list,
    mid_list,
    top_list,
    upper_list,
    positions,
    leaf_cell,
):
    domains, subs = lax.axis_size("dom"), lax.axis_size("sub")
    slab = fine_partial.shape[2]
    mid = slab // 8
    top = slab // 64
    slots, coeffs = interaction_ops.shape[:2]
    particles = leaf_cell.shape[0]
    rows = round_up(coeffs, 24)
    depth = round_up(slots, 16)
    parts = round_up(coeffs, 8) // 8
    picked = (rows + 1) * (depth + 8)
    spread = 3 * mid
    tops = top * domains
    coarse_rows = round_up(mid + top + 1, 8)
    counts = (slab, mid, top, spread, tops)
    width = round_up(spread + tops + tops // 8, LANES)
    others = max(subs - 1, 1)
    wide = 2 * LANES
    f32, bf16, i32 = jnp.float32, jnp.bfloat16, jnp.int32
    table = jnp.asarray(exponents(), i32)
    table = jnp.pad(table, ((0, rows - coeffs), (0, LANES - 3)))
    shapes = [
        ((coeffs, slab), f32),
        ((8, coeffs, coeffs), f32),
        ((8, coeffs, coeffs), f32),
        ((slots, slab), i32),
        ((mid, slots), i32),
        ((top, slots), i32),
        ((upper_list.shape[1], slots), i32),
        ((1, particles), i32),
        ((3, particles), f32),
        ((rows, LANES), i32),
        ((parts, coeffs, 8, slots), f32),
        ((rows, 8 * wide), bf16),
        ((rows, 8 * wide), bf16),
        ((rows, 8 * wide), bf16),
        ((rows, 8 * wide), bf16),
        ((mid, wide), f32),
        ((top, wide), f32),
        ((others, coeffs, slab), f32),
        ((others, mid, wide), f32),
        ((coeffs, slab), f32),
        ((mid, wide), f32),
        ((coeffs, slab), f32),
        ((coeffs, slab), f32),
        ((LANES, wide), f32),
        ((domains * subs, top, wide), f32),
        ((round_up(tops, LANES), wide), f32),
        ((2, depth, LANES), f32),
        ((LANES, LANES), f32),
        ((3, rows, wide), bf16),
        ((rows, 2 * width), bf16),
        ((picked, LANES), f32),
        ((picked, LANES), f32),
        ((rows, LANES), f32),
        ((coarse_rows, wide), f32),
        ((others, rows, LANES), f32),
        ((others, coarse_rows, wide), f32),
        ((slab, particles), bf16),
        ((rows, particles), f32),
        ((rows, width), f32),
    ]
    semaphores = [(24,), (parts,)] + 2 * [(2 * others,)] + 2 * [(4,)] + 2 * [()]
    semaphores += 2 * [(2 * others,)]
    vmem = pl.BlockSpec(memory_space=pltpu.VMEM)
    local_fine, potential = pl.pallas_call(
        functools.partial(step_kernel, domains, subs, counts),
        in_specs=[pl.BlockSpec(memory_space=pltpu.HBM)] * 11,
        out_specs=[vmem] * 2,
        out_shape=[
            jax.ShapeDtypeStruct((coeffs, slab), f32),
            jax.ShapeDtypeStruct((1, particles), f32),
        ],
        scratch_shapes=[pltpu.VMEM(*one) for one in shapes]
        + [pltpu.SemaphoreType.DMA(one) if one else pltpu.SemaphoreType.DMA for one in semaphores],
        compiler_params=pltpu.CompilerParams(
            collective_id=0, has_side_effects=True, vmem_limit_bytes=67_043_328
        ),
    )(
        jnp.transpose(fine_partial, (1, 0, 2)),
        jnp.transpose(upward_ops, (1, 0, 2)),
        jnp.transpose(interaction_ops, (1, 2, 0)),
        jnp.transpose(downward_ops, (1, 0, 2)),
        fine_list,
        jnp.transpose(mid_list),
        jnp.transpose(top_list),
        jnp.transpose(upper_list),
        leaf_cell[None],
        positions,
        table,
    )
    return deliver(local_fine, potential)


def deliver_kernel(local_ref, potential_ref, local_out, potential_out, local, potential, sems):
    ways = ((local_ref, local, local_out), (potential_ref, potential, potential_out))
    loads = [pltpu.make_async_copy(way[0], way[1], sems.at[k]) for k, way in enumerate(ways)]
    stores = [pltpu.make_async_copy(way[1], way[2], sems.at[2 + k]) for k, way in enumerate(ways)]
    for one in loads:
        one.start()
    for load, store in zip(loads, stores):
        load.wait()
        store.start()
    for one in stores:
        one.wait()


def deliver(local_fine, potential):
    shapes = (local_fine.shape, potential.shape)
    local_fine, potential = pl.pallas_call(
        deliver_kernel,
        in_specs=[pl.BlockSpec(memory_space=pltpu.HBM)] * 2,
        out_specs=[pl.BlockSpec(memory_space=pltpu.HBM)] * 2,
        out_shape=[jax.ShapeDtypeStruct(one, jnp.float32) for one in shapes],
        scratch_shapes=[pltpu.VMEM(one, jnp.float32) for one in shapes]
        + [pltpu.SemaphoreType.DMA((4,))],
        compiler_params=pltpu.CompilerParams(vmem_limit_bytes=67_043_328),
    )(local_fine, potential)
    return local_fine, potential[0]


def solution(mesh):
    placed = (
        P("sub", None, "dom"),
        P(),
        P("sub", None, None),
        P(),
        P("sub", "dom"),
        P("sub", "dom"),
        P("sub", "dom"),
        P("sub", None),
        P(None, ("dom", "sub")),
        P(("dom", "sub")),
    )
    return jax.shard_map(
        shards,
        mesh=mesh,
        in_specs=placed,
        out_specs=(P(None, "dom"), P(("dom", "sub"))),
        check_vma=False,
    )
```

```python
import functools

import jax
import jax.numpy as jnp
from jax import lax
from jax.experimental import pallas as pl
from jax.experimental.pallas import tpu as pltpu
from jax.sharding import PartitionSpec as P

ORDER = 8
LANES = 128


def round_up(count, unit):
    return -(-count // unit) * unit


def exponents():
    entries = []
    for degree in range(ORDER + 1):
        for along_x in range(degree, -1, -1):
            for along_y in range(degree - along_x, -1, -1):
                entries.append((along_x, along_y, degree - along_x - along_y))
    return entries


def halves(value):
    high = value.astype(jnp.bfloat16)
    low = (value - high.astype(jnp.float32)).astype(jnp.bfloat16)
    return high, low


def one_hot(row, count):
    places = lax.broadcasted_iota(jnp.int32, (count, row.shape[1]), 0)
    return jnp.where(places == row, 1.0, 0.0).astype(jnp.bfloat16)


def matmul(left, right):
    return jnp.dot(left, right, preferred_element_type=jnp.float32)


def one_hot_blocks(row, blocks):
    places = lax.broadcasted_iota(jnp.int32, (LANES, LANES), 0)
    places = places.astype(jnp.float32).astype(jnp.bfloat16)
    pieces = []
    for m in blocks:
        wanted = jnp.broadcast_to(row - float(LANES * m), (LANES, LANES)).astype(jnp.bfloat16)
        one, zero = jnp.ones((), jnp.bfloat16), jnp.zeros((), jnp.bfloat16)
        pieces.append(jnp.where(places == wanted, one, zero))
    return jnp.concatenate(pieces, axis=0)


def operator_copy(ops_ref, stage, arrived, part):
    coeffs = ops_ref.shape[0]
    count = min(8, coeffs - 8 * part)
    return pltpu.make_async_copy(
        ops_ref.at[:, pl.ds(8 * part, count), :],
        stage.at[part, :, pl.ds(0, count), :],
        arrived.at[part],
    )


def raise_level(moments, ops_high, ops_low):
    rows, width = moments.shape
    parents = round_up(width // 8, LANES)
    high, low = halves(moments)
    source = lax.broadcasted_iota(jnp.int32, (width, 8 * parents), 0)
    target = lax.broadcasted_iota(jnp.int32, (width, 8 * parents), 1)
    wanted = 8 * (target % parents) + target // parents
    chosen = jnp.where(source == wanted, 1.0, 0.0).astype(jnp.bfloat16)
    both = matmul(jnp.concatenate([high, low], axis=0), chosen)
    filler = jnp.zeros((2 * LANES - rows, parents), jnp.float32)
    stacks = []
    for first in (0, rows):
        pieces = []
        for o in range(8):
            pieces += [both[first : first + rows, o * parents : (o + 1) * parents], filler]
        stacks.append(jnp.concatenate(pieces, axis=0).astype(jnp.bfloat16))
    value = matmul(ops_high[...], stacks[0]) + matmul(ops_high[...], stacks[1])
    return value + matmul(ops_low[...], stacks[0])


def transfer(source, target, sems, index, place):
    return pltpu.make_async_remote_copy(
        src_ref=source,
        dst_ref=target,
        send_sem=sems[0].at[index],
        recv_sem=sems[1].at[index],
        device_id=place,
        device_id_type=pl.DeviceIdType.MESH,
    )


def total_of(first, others):
    for k in range(others.shape[0]):
        first = first + others[k]
    return first


def padded(value, height, width):
    below, beside = height - value.shape[0], width - value.shape[1]
    if beside:
        filler = jnp.zeros((value.shape[0], beside), value.dtype)
        value = jnp.concatenate([value, filler], axis=1)
    if below:
        value = jnp.concatenate([value, jnp.zeros((below, width), value.dtype)], axis=0)
    return value


def fill_octant(ops, octant, high_ref, low_ref):
    coeffs = ops.shape[1]
    at = 2 * LANES * octant
    high_ref[:coeffs, at : at + coeffs], low_ref[:coeffs, at : at + coeffs] = halves(ops[octant])


def spread_level(expansions, offset, ops_high, ops_low):
    rows = expansions.shape[0]
    parent = lax.broadcasted_iota(jnp.int32, (LANES, LANES), 0)
    child = lax.broadcasted_iota(jnp.int32, (LANES, LANES), 1) + offset
    copied = jnp.where(child // 8 == parent, 1.0, 0.0).astype(jnp.bfloat16)
    high, low = halves(expansions)
    both = matmul(jnp.concatenate([high, low], axis=0), copied).astype(jnp.bfloat16)
    wide = jnp.concatenate([both[:rows], both[rows:]], axis=1).astype(jnp.float32)
    wide = padded(wide, 2 * LANES, 2 * LANES)
    octant = (lax.broadcasted_iota(jnp.int32, wide.shape, 1) % LANES + offset) % 8
    pieces = [jnp.where(octant == o, wide, 0.0).astype(jnp.bfloat16) for o in range(8)]
    right = jnp.concatenate(pieces, axis=0)
    first = matmul(ops_high[...], right)
    second = matmul(ops_low[...], right[:, :LANES])
    return first[:, :LANES] + first[:, LANES:] + second


def pick_slots(list_ref, tables, picked, rows, blocks, repeats, adding):
    depth = list_ref.shape[0]
    stride = picked.shape[0] // (rows + 1)
    batch = 32 if depth % 32 == 0 else 16

    def step(number, carry):
        base = pl.multiple_of(number * batch, batch)
        for slot in range(0, batch, 2):
            pair = [
                one_hot_blocks(list_ref[pl.ds(base + slot + m, 1), :], blocks) for m in range(2)
            ]
            chosen = jnp.concatenate(pair, axis=1)
            chosen = jnp.concatenate([chosen] * repeats, axis=0)
            value = matmul(tables[0][...], chosen)
            for table in tables[1:]:
                value += matmul(table[...], chosen)
            for m in range(2):
                at = pl.ds(base + slot + m, rows, stride)
                part = value[:, m * LANES : (m + 1) * LANES]
                picked[at, :] = picked[at, :] + part if adding else part
        return carry

    lax.fori_loop(0, depth // batch, step, 0)


def contract(stage, fine_picked, coarse_picked, rows, depth):
    coeffs, slots = stage.shape[1], stage.shape[3]
    stride = fine_picked.shape[0] // (rows + 1)
    below = jnp.zeros((LANES - depth, 2 * LANES), jnp.bfloat16)
    total = None
    for first in range(0, coeffs, 24):
        left = []
        right = []
        for term in range(first, min(first + 24, coeffs)):
            block = stage.at[term // 8].reshape(coeffs * 8, slots)
            op_high, op_low = halves(padded(block[pl.ds(term % 8, coeffs, 8), :], rows, LANES))
            place = pl.ds(term * stride, depth)
            data = jnp.concatenate([fine_picked[place, :], coarse_picked[place, :]], axis=1)
            high, low = halves(data)
            high = jnp.concatenate([high, below], axis=0)
            low = jnp.concatenate([low, below], axis=0)
            left += [op_high, op_high, op_low]
            right += [high, low, high]
        product = matmul(jnp.concatenate(left, axis=1), jnp.concatenate(right, axis=0))
        total = product if total is None else total + product
    return total


def step_kernel(
    domains, subs, counts, partial_ref, upward_ref, ops_ref, downward_ref, fine_ref, mid_ref,
    top_list_ref, upper_ref, leaf_ref, position_ref, exponent_ref,
    local_out, potential_out,
    mine, upward, downward, fine_in, mid_in, top_in, upper_in, leaves, positions, powers,
    stage, up_high, up_low, down_high, down_low, mids, top_ref, parts, mid_parts, sums,
    mid_sums, low, high, mid_rows, tops, top_rows, lists, turned_lists, fine_table,
    coarse_table, fine_picked, coarse_picked, fine_terms, coarse_terms, fine_parts,
    coarse_parts, chosen_ref, factors_ref, coarse_ref,
    load, arrived_ops, part_send, part_recv, side_send, side_recv, top_send, top_recv,
    term_send, term_recv,
):
    domain, sub = lax.axis_index("dom"), lax.axis_index("sub")
    slab, mid, top, spread, all_tops = counts
    count = domains * subs
    flat = domain * subs + sub
    coeffs, cells = mine.shape
    rows = up_high.shape[0]
    depth = lists.shape[1]
    slots = fine_in.shape[0]
    particles = leaves.shape[1]
    width = coarse_table.shape[1] // 2
    part_sems, side_sems = (part_send, part_recv), (side_send, side_recv)
    term_sems = (term_send, term_recv)

    loads = [pltpu.make_async_copy(partial_ref.at[:, 0, :], mine, load.at[0])]
    for o in range(8):
        loads.append(
            pltpu.make_async_copy(upward_ref.at[:, o, :], upward.at[o], load.at[1 + o])
        )
    for k, (source, target) in enumerate(
        (
            (fine_ref, fine_in), (mid_ref, mid_in), (top_list_ref, top_in),
            (upper_ref, upper_in), (leaf_ref, leaves), (position_ref, positions),
            (exponent_ref, powers),
        )
    ):
        loads.append(pltpu.make_async_copy(source, target, load.at[9 + k]))
    downs = [
        pltpu.make_async_copy(downward_ref.at[:, o, :], downward.at[o], load.at[16 + o])
        for o in range(8)
    ]
    for one in loads:
        one.start()
    barrier = pltpu.get_barrier_semaphore()

    def peer(offset):
        place = lax.rem(flat + offset, count)
        return {"dom": place // subs, "sub": lax.rem(place, subs)}

    def greet(offset, carry):
        pl.semaphore_signal(
            barrier, inc=1, device_id=peer(offset), device_id_type=pl.DeviceIdType.MESH
        )
        return carry

    mid_rows[...] = jnp.zeros_like(mid_rows)
    top_rows[...] = jnp.zeros_like(top_rows)
    lax.fori_loop(1, count, greet, 0)
    for ref in (up_high, up_low, down_high, down_low):
        ref[...] = jnp.zeros_like(ref)
    for o in range(8):
        loads[1 + o].wait()
        fill_octant(upward, o, up_high, up_low)
    loads[0].wait()
    for one in downs:
        one.start()
    for part in range(stage.shape[0]):
        operator_copy(ops_ref, stage, arrived_ops, part).start()
    mid_moments = raise_level(padded(mine[...], rows, cells), up_high, up_low)
    top_moments = raise_level(mid_moments, up_high, up_low)
    both = mid_moments + pltpu.roll(top_moments, mid, 1)
    turned = jnp.transpose(padded(both, 2 * LANES, LANES))
    mids[...] = turned[:mid]
    top_ref[...] = turned[mid : mid + top]
    tops[count - 1] = top_ref[...]
    pl.semaphore_wait(barrier, count - 1)

    def send(offset, carry):
        pltpu.make_async_remote_copy(
            src_ref=top_ref,
            dst_ref=tops.at[offset - 1],
            send_sem=top_send,
            recv_sem=top_recv,
            device_id=peer(offset),
            device_id_type=pl.DeviceIdType.MESH,
        ).start()
        return carry

    sub_peers = [{"dom": domain, "sub": lax.rem(sub + k + 1, subs)} for k in range(subs - 1)]
    copies = []
    for k, place in enumerate(sub_peers):
        copies.append(transfer(mine, parts.at[k], part_sems, 2 * k, place))
        copies.append(transfer(mids, mid_parts.at[k], part_sems, 2 * k + 1, place))
    for one in copies:
        one.start()
    lax.fori_loop(1, count, send, 0)

    for one in loads[9:]:
        one.wait()

    def place_in(sources, offset):
        return jnp.where(sources >= 0, sources + offset, -1).astype(jnp.float32)

    lists[0, :slots] = place_in(fine_in[...], slab - domain * slab)
    lists[0, slots:] = jnp.full((depth - slots, LANES), -1.0, jnp.float32)
    turned_lists[...] = jnp.full_like(turned_lists, -1.0)
    start = 0
    for part in (
        place_in(mid_in[...], mid - domain * mid),
        place_in(top_in[...], spread),
        place_in(upper_in[pl.ds(domain * top // 8, 1), :], spread + all_tops),
    ):
        turned_lists[start : start + part.shape[0], :slots] = part
        start += part.shape[0]
    lists[1] = jnp.transpose(turned_lists[...])[:depth]

    lane = lax.broadcasted_iota(jnp.int32, (rows, LANES), 1)
    takes = []
    for axis in range(3):
        taken = (lane < 48) & (lane % 16 == powers[:, axis : axis + 1])
        takes.append(jnp.where(taken, 1.0, 0.0).astype(jnp.bfloat16))
    power = lax.broadcasted_iota(jnp.int32, (16, 2 * LANES), 0)
    power_bits = [(power // bit) % 2 == 1 for bit in (1, 2, 4, 8)]
    below = jnp.zeros((LANES - 48, 2 * LANES), jnp.bfloat16)

    def factor(number, carry):
        span = pl.ds(pl.multiple_of(number * 2 * LANES, 2 * LANES), 2 * LANES)
        chosen_ref[:, span] = one_hot(leaves[:, span] - domain * slab, cells)
        value = None
        for axis in range(3):
            base = positions[axis : axis + 1, span]
            raised = jnp.ones((16, 2 * LANES), jnp.float32)
            for bit in power_bits:
                raised = raised * jnp.where(bit, base, 1.0)
                base = base * base
            first, rest = halves(raised)
            left_over = raised - first.astype(jnp.float32) - rest.astype(jnp.float32)
            stack = jnp.concatenate(
                [first, rest, left_over.astype(jnp.bfloat16), below], axis=0
            )
            taken = matmul(takes[axis], stack)
            value = taken if value is None else value * taken
        factors_ref[:, span] = value
        return carry

    lax.fori_loop(0, particles // (2 * LANES), factor, 0)
    for o in range(8):
        downs[o].wait()
        fill_octant(downward, o, down_high, down_low)
    for one in copies:
        one.wait()
    sums[...] = total_of(mine[...], parts)
    mid_sums[...] = total_of(mids[...], mid_parts)
    copies = []
    for index, (target, first, move) in enumerate(((low, 0, 1), (high, 2 * mid, domains - 1))):
        place = {"dom": lax.rem(domain + move, domains), "sub": sub}
        copies.append(transfer(sums, target, side_sems, 2 * index, place))
        rows_there = mid_rows.at[pl.ds(first, mid)]
        copies.append(transfer(mid_sums, rows_there, side_sems, 2 * index + 1, place))
    for one in copies:
        one.start()

    def split(block):
        return halves(padded(block, rows, LANES))

    fine_table[0, :, :LANES], fine_table[0, :, LANES:] = split(sums[...])
    pick_slots(lists.at[0], [fine_table.at[0]], fine_picked, rows, (1,), 2, False)
    arrived = tops.at[pl.ds(0, count - 1)]
    pltpu.make_async_copy(arrived, arrived, top_recv).wait()

    def gather(offset, carry):
        source = lax.rem(flat + count - offset, count) // subs
        slot = lax.rem(offset + count - 1, count)
        for r in range(top):
            at = pl.ds(source * top + r, 1)
            top_rows[at, :] = top_rows[at, :] + tops[slot, r : r + 1, :]
        return carry

    lax.fori_loop(0, count, gather, 0)

    def shifted(value, amount):
        value = padded(value, rows, width)
        return pltpu.roll(value, amount, 1) if amount else value

    top_moments = jnp.transpose(top_rows[...])[:rows]
    coarse = shifted(top_moments, spread)
    coarse += shifted(raise_level(top_moments, up_high, up_low), spread + all_tops)
    coarse_ref[...] = coarse
    for one in copies:
        one.wait()
    fine_table[1, :, :LANES], fine_table[2, :, :LANES] = split(low[...])
    fine_table[1, :, LANES:], fine_table[2, :, LANES:] = split(high[...])
    sides = [fine_table.at[1], fine_table.at[2]]
    pick_slots(lists.at[0], sides, fine_picked, rows, (0, 2), 1, True)

    mid_rows[mid : 2 * mid] = mid_sums[...]
    coarse = coarse_ref[...] + shifted(jnp.transpose(mid_rows[...])[:rows], 0)
    coarse_table[:, :width], coarse_table[:, width:] = halves(coarse)
    blocks = tuple(range(width // LANES))
    pick_slots(lists.at[1], [coarse_table], coarse_picked, rows, blocks, 2, False)

    for part in range(stage.shape[0]):
        operator_copy(ops_ref, stage, arrived_ops, part).wait()
    total = contract(stage, fine_picked, coarse_picked, rows, depth)
    fine_terms[...] = total[:, :LANES]
    turned = jnp.transpose(padded(total[:, LANES:], 2 * LANES, LANES))
    coarse_terms[...] = turned[: coarse_terms.shape[0]]
    coarse_copies = []
    fine_copies = []
    for k, place in enumerate(sub_peers):
        coarse_copies.append(
            transfer(coarse_terms, coarse_parts.at[k], term_sems, 2 * k, place)
        )
        fine_copies.append(transfer(fine_terms, fine_parts.at[k], term_sems, 2 * k + 1, place))
    for one in coarse_copies + fine_copies:
        one.start()
    for one in coarse_copies:
        one.wait()
    coarse = jnp.transpose(padded(total_of(coarse_terms[...], coarse_parts), LANES, 2 * LANES))
    coarse = coarse[:rows]
    lane = lax.broadcasted_iota(jnp.int32, coarse.shape, 1)

    def columns(first, number):
        value = pltpu.roll(coarse, LANES - first, 1) if first else coarse
        return jnp.where(lane < number, value, 0.0)

    local = columns(mid + top, 1)
    local = columns(mid, top) + spread_level(local, domain * top % 8, down_high, down_low)
    local = jnp.where(lane < top, local, 0.0)
    local = columns(0, mid) + spread_level(local, 0, down_high, down_low)
    local = spread_level(local, 0, down_high, down_low)
    for one in fine_copies:
        one.wait()
    local = total_of(fine_terms[...], fine_parts) + local
    local_out[...] = local[:coeffs]
    table = jnp.concatenate(halves(local), axis=1)
    for start in range(0, particles, 2 * LANES):
        span = slice(start, start + 2 * LANES)
        chosen = chosen_ref[:, span]
        value = matmul(table, jnp.concatenate([chosen, chosen], axis=0)) * factors_ref[:, span]
        potential_out[:, span] = jnp.sum(value, axis=0, keepdims=True)
    pltpu.make_async_copy(arrived, arrived, top_send).wait()


def shards(
    fine_partial,
    upward_ops,
    interaction_ops,
    downward_ops,
    fine_list,
    mid_list,
    top_list,
    upper_list,
    positions,
    leaf_cell,
):
    domains, subs = lax.axis_size("dom"), lax.axis_size("sub")
    slab = fine_partial.shape[2]
    mid = slab // 8
    top = slab // 64
    slots, coeffs = interaction_ops.shape[:2]
    particles = leaf_cell.shape[0]
    rows = round_up(coeffs, 24)
    depth = round_up(slots, 16)
    parts = round_up(coeffs, 8) // 8
    picked = (rows + 1) * (depth + 8)
    spread = 3 * mid
    tops = top * domains
    coarse_rows = round_up(mid + top + 1, 8)
    counts = (slab, mid, top, spread, tops)
    width = round_up(spread + tops + tops // 8, LANES)
    others = max(subs - 1, 1)
    wide = 2 * LANES
    f32, bf16, i32 = jnp.float32, jnp.bfloat16, jnp.int32
    table = jnp.asarray(exponents(), i32)
    table = jnp.pad(table, ((0, rows - coeffs), (0, LANES - 3)))
    shapes = [
        ((coeffs, slab), f32),
        ((8, coeffs, coeffs), f32),
        ((8, coeffs, coeffs), f32),
        ((slots, slab), i32),
        ((mid, slots), i32),
        ((top, slots), i32),
        ((upper_list.shape[1], slots), i32),
        ((1, particles), i32),
        ((3, particles), f32),
        ((rows, LANES), i32),
        ((parts, coeffs, 8, slots), f32),
        ((rows, 8 * wide), bf16),
        ((rows, 8 * wide), bf16),
        ((rows, 8 * wide), bf16),
        ((rows, 8 * wide), bf16),
        ((mid, wide), f32),
        ((top, wide), f32),
        ((others, coeffs, slab), f32),
        ((others, mid, wide), f32),
        ((coeffs, slab), f32),
        ((mid, wide), f32),
        ((coeffs, slab), f32),
        ((coeffs, slab), f32),
        ((LANES, wide), f32),
        ((domains * subs, top, wide), f32),
        ((round_up(tops, LANES), wide), f32),
        ((2, depth, LANES), f32),
        ((LANES, LANES), f32),
        ((3, rows, wide), bf16),
        ((rows, 2 * width), bf16),
        ((picked, LANES), f32),
        ((picked, LANES), f32),
        ((rows, LANES), f32),
        ((coarse_rows, wide), f32),
        ((others, rows, LANES), f32),
        ((others, coarse_rows, wide), f32),
        ((slab, particles), bf16),
        ((rows, particles), f32),
        ((rows, width), f32),
    ]
    semaphores = [(24,), (parts,)] + 2 * [(2 * others,)] + 2 * [(4,)] + 2 * [()]
    semaphores += 2 * [(2 * others,)]
    vmem = pl.BlockSpec(memory_space=pltpu.VMEM)
    local_fine, potential = pl.pallas_call(
        functools.partial(step_kernel, domains, subs, counts),
        in_specs=[pl.BlockSpec(memory_space=pltpu.HBM)] * 11,
        out_specs=[vmem] * 2,
        out_shape=[
            jax.ShapeDtypeStruct((coeffs, slab), f32),
            jax.ShapeDtypeStruct((1, particles), f32),
        ],
        scratch_shapes=[pltpu.VMEM(*one) for one in shapes]
        + [pltpu.SemaphoreType.DMA(one) if one else pltpu.SemaphoreType.DMA for one in semaphores],
        compiler_params=pltpu.CompilerParams(
            collective_id=0, has_side_effects=True, vmem_limit_bytes=67_043_328
        ),
    )(
        jnp.transpose(fine_partial, (1, 0, 2)),
        jnp.transpose(upward_ops, (1, 0, 2)),
        jnp.transpose(interaction_ops, (1, 2, 0)),
        jnp.transpose(downward_ops, (1, 0, 2)),
        fine_list,
        jnp.transpose(mid_list),
        jnp.transpose(top_list),
        jnp.transpose(upper_list),
        leaf_cell[None],
        positions,
        table,
    )
    return deliver(local_fine, potential)


def deliver_kernel(local_ref, potential_ref, local_out, potential_out, local, potential, sems):
    ways = ((local_ref, local, local_out), (potential_ref, potential, potential_out))
    loads = [pltpu.make_async_copy(way[0], way[1], sems.at[k]) for k, way in enumerate(ways)]
    stores = [pltpu.make_async_copy(way[1], way[2], sems.at[2 + k]) for k, way in enumerate(ways)]
    for one in loads:
        one.start()
    for load, store in zip(loads, stores):
        load.wait()
        store.start()
    for one in stores:
        one.wait()


def deliver(local_fine, potential):
    shapes = (local_fine.shape, potential.shape)
    local_fine, potential = pl.pallas_call(
        deliver_kernel,
        in_specs=[pl.BlockSpec(memory_space=pltpu.HBM)] * 2,
        out_specs=[pl.BlockSpec(memory_space=pltpu.HBM)] * 2,
        out_shape=[jax.ShapeDtypeStruct(one, jnp.float32) for one in shapes],
        scratch_shapes=[pltpu.VMEM(one, jnp.float32) for one in shapes]
        + [pltpu.SemaphoreType.DMA((4,))],
        compiler_params=pltpu.CompilerParams(vmem_limit_bytes=67_043_328),
    )(local_fine, potential)
    return local_fine, potential[0]


def solution(mesh):
    placed = (
        P("sub", None, "dom"),
        P(),
        P("sub", None, None),
        P(),
        P("sub", "dom"),
        P("sub", "dom"),
        P("sub", "dom"),
        P("sub", None),
        P(None, ("dom", "sub")),
        P(("dom", "sub")),
    )
    return jax.shard_map(
        shards,
        mesh=mesh,
        in_specs=placed,
        out_specs=(P(None, "dom"), P(("dom", "sub"))),
        check_vma=False,
    )
```
